32 devices in a mesh: row: 4 (over y, core), col: 8 (over z, x).
Axes of the slice: x: 2, y: 2, z: 4, core: 2. Of those that a mesh axis runs over, the one named last changes fastest.
Arguments:
- matrix: bfloat16 [6144, 6144], P('row', 'col'), as said below
- polar_factor: bfloat16 [6144, 6144], P('row', 'col'), as said below
- start_basis: bfloat16 [6144, 6144], P('row', 'col'), may hold values from -0.078125 to 0.078125
Outputs:
- gram_halves: float32 [3072, 6144], P('row', 'col')
- projected: float32 [3072, 6144], P('row', 'col')
The draws below stay inside these ranges and needn't reach their ends.
Inputs may be any that keep to these rules, and one draw needn't show every extreme that they name: `matrix`: symmetric. `polar_factor`: symmetric.
All inputs are finite; a program needn't handle non-finite values.
Results may differ from the reference program's by a relative error of at most 0.017.
Values may be sent and summed in bfloat16 or wider, within the bound.
A program may use at most 128 MiB of HBM per device.

```python
import jax
import jax.numpy as jnp
from jax import lax

N = 6144
K = 3072
BLOCK_ROWS = 1536
HALF_BLOCK = 384
N_ROW = 4
N_COL = 8


def spectral_parts(key):
    base = jax.random.fold_in(key, 7)
    first, second, third = jax.random.split(base, 3)
    normal_draw = jax.random.normal(first, (N, N), jnp.float32)
    orthogonal, unused = jnp.linalg.qr(normal_draw)
    magnitude = jax.random.uniform(second, (N,), jnp.float32, 0.2, 2.0)
    signs = jnp.where(jnp.arange(N) < K, 1.0, -1.0).astype(jnp.float32)
    errors = jax.random.uniform(third, (N,), jnp.float32, 0.0, 0.3)
    return (orthogonal, signs * magnitude, signs * (1.0 - errors))


def symmetric_from(orthogonal, values):
    built = jnp.dot(orthogonal * values[None, :], orthogonal.T, precision=lax.Precision.HIGHEST)
    return 0.5 * (built + built.T)


def draw_matrix(key, part):
    orthogonal, eigen, polar = spectral_parts(key)
    return symmetric_from(orthogonal, eigen).astype(jnp.bfloat16)


def draw_polar_factor(key, part):
    orthogonal, eigen, polar = spectral_parts(key)
    return symmetric_from(orthogonal, polar).astype(jnp.bfloat16)


def block_scale(own_key, shape, pieces, smallest, top_value):
    gain, own = 1.0, jax.random.fold_in(own_key, 6)
    for dim, blocks in pieces:
        heights = jnp.exp(jax.random.uniform(jax.random.fold_in(own, dim), (blocks,), jnp.float32, smallest / len(pieces), top_value / len(pieces)))
        gain = gain * jnp.repeat(heights, shape[dim] // blocks).reshape([-1 if axis == dim else 1 for axis in range(len(shape))])
    return gain


def noise(stream_key, dims, width, bound, cuts=(), dtype=jnp.bfloat16):
    factor_of = block_scale(stream_key, dims, cuts, -0.22, 0.18) if cuts else 1.0
    array = jax.random.normal(stream_key, dims, jnp.float32) * width * factor_of
    return jnp.minimum(jnp.maximum(array, -bound), bound).astype(dtype)


def setup_inputs(seed: int = 0) -> dict:
    splits = jax.random.split(jax.random.key(seed), 4)
    matrix = draw_matrix(jax.random.fold_in(splits[3], 71), 0)
    polar_factor = draw_polar_factor(jax.random.fold_in(splits[3], 71), 0)
    start_basis = noise(splits[2], (N, 2 * K), N ** -0.5, 0.078125, ((0, 4), (1, 8)))
    return dict(matrix=matrix, polar_factor=polar_factor, start_basis=start_basis)


def add_block(running, blocks):
    left, right = blocks
    term = jnp.dot(left.T.astype(jnp.float32), right.astype(jnp.float32), preferred_element_type=jnp.float32).astype(jnp.bfloat16)
    term = lax.optimization_barrier(term)
    return (running + term.astype(jnp.float32), None)

def reference(matrix, polar_factor, start_basis):
    product = jnp.dot(polar_factor.astype(jnp.float32), start_basis.astype(jnp.float32), preferred_element_type=jnp.float32)
    signs = jnp.where(jnp.arange(2 * K) // HALF_BLOCK % 2 == 0, 1.0, -1.0).astype(jnp.float32)
    basis = ((start_basis.astype(jnp.float32) + signs * product) * 0.5).astype(jnp.bfloat16)
    image = jnp.dot(matrix.astype(jnp.float32), basis.astype(jnp.float32), preferred_element_type=jnp.float32).astype(jnp.bfloat16)
    basis_split = basis.reshape(N, N_COL, 2, HALF_BLOCK)
    image_split = image.reshape(N, N_COL, 2, HALF_BLOCK)
    grams = []
    projections = []
    for which in range(2):
        basis_half = basis_split[:, :, which, :].reshape(N, K)
        image_half = image_split[:, :, which, :].reshape(N, K)
        joined = jnp.concatenate([basis_half, image_half], axis=1)
        left_blocks = basis_half.reshape(N_ROW, BLOCK_ROWS, K)
        right_blocks = joined.reshape(N_ROW, BLOCK_ROWS, 2 * K)
        summed, unused = lax.scan(add_block, jnp.zeros((K, 2 * K), jnp.float32), (left_blocks, right_blocks))
        grams.append(summed[:, :K].reshape(K, N_COL, HALF_BLOCK))
        projections.append(summed[:, K:].reshape(K, N_COL, HALF_BLOCK))
    gram_halves = jnp.stack(grams, axis=2).reshape(K, 2 * K)
    projected = jnp.stack(projections, axis=2).reshape(K, 2 * K)
    return (gram_halves, projected)
```

```python
import jax
import jax.numpy as jnp
from jax import lax
from jax.sharding import PartitionSpec as P


def ring_member(place, count):
    return jnp.where(place < count // 2, 2 * place, 2 * (count - 1 - place) + 1)


def ring_pairs(count):
    order = list(range(0, count, 2)) + list(range(count - 1, 0, -2))
    up = [(order[i], order[(i + 1) % count]) for i in range(count)]
    return up, [(b, a) for a, b in up]


def ring(first, second, count, consume, state):
    here = lax.axis_index("col")
    place = jnp.where(here % 2 == 0, here // 2, count - 1 - here // 2)
    up, down = ring_pairs(count)
    seen = []
    for step in range(count):
        if step < count - 1:
            next_first = lax.ppermute(first, "col", up)
            next_second = lax.ppermute(second, "col", down)
        owner_first = ring_member(lax.rem(place - step + count, count), count)
        owner_second = ring_member(lax.rem(place + step, count), count)
        state = consume(state, first, owner_first, second, owner_second)
        seen.append(first)
        first, second = next_first, next_second
    return state, seen


def block_row_product(block, columns, count, half_rows):
    depth = block.shape[1]

    def consume(state, top, owner_top, bottom, owner_bottom):
        pieces = []
        for total, piece, owner in ((state[0], top, owner_top), (state[1], bottom, owner_bottom)):
            rows = lax.dynamic_slice_in_dim(columns, owner * depth, depth, 0)
            term = jnp.dot(piece, rows, preferred_element_type=jnp.float32)
            pieces.append(term if total is None else total + term)
        return tuple(pieces)

    return ring(block[:half_rows], block[half_rows:], count, consume, (None, None))


def transposed_product(left, right):
    return lax.dot_general(
        left, right, (((0,), (0,)), ((), ())), preferred_element_type=jnp.float32
    )


def per_device(matrix, polar_factor, start_basis):
    local_rows, width = start_basis.shape
    count = lax.axis_size("col")
    half = width // 2
    half_rows = local_rows // 2
    sign = jnp.where(jnp.arange(width) < half, 1.0, -1.0).astype(jnp.float32)

    start_cols = lax.all_gather(start_basis, "row", axis=0, tiled=True)
    (top, bottom), _ = block_row_product(polar_factor, start_cols, count, half_rows)
    product = jnp.concatenate([top, bottom], axis=0)
    basis = ((start_basis.astype(jnp.float32) + sign * product) * 0.5).astype(jnp.bfloat16)
    basis_cols = lax.all_gather(basis, "row", axis=0, tiled=True)

    def keep(state, first, owner_first, second, owner_second):
        return (
            lax.dynamic_update_slice_in_dim(state[0], first, owner_first * half, 1),
            lax.dynamic_update_slice_in_dim(state[1], second, owner_second * half, 1),
        )

    empty = jnp.zeros((local_rows, half * count), jnp.bfloat16)
    lefts, seen = ring(basis[:, :half], basis[:, half:], count, keep, (empty, empty))

    matrix, _ = lax.optimization_barrier((matrix, seen[count // 2]))
    halves, _ = block_row_product(matrix, basis_cols, count, half_rows)
    image = jnp.concatenate(halves, axis=0).astype(jnp.bfloat16)

    def summed(right):
        terms = [
            transposed_product(lefts[0], right[:, :half]),
            transposed_product(lefts[1], right[:, half:]),
        ]
        return lax.psum_scatter(
            jnp.concatenate(terms, axis=1).astype(jnp.bfloat16),
            "row",
            scatter_dimension=0,
            tiled=True,
        ).astype(jnp.float32)

    return summed(basis), summed(image)


def solution(mesh):
    return jax.shard_map(
        per_device,
        mesh=mesh,
        in_specs=(P("row", "col"), P("row", "col"), P("row", "col")),
        out_specs=(P("row", "col"), P("row", "col")),
        check_vma=False,
    )
```
